256 devices in a mesh: pts: 32 (over z, x_hi, core), bond: 8 (over x_lo, y).
Axes of the slice: x: 4 (x_hi: 2, x_lo: 2; x = x_hi * 2 + x_lo), y: 4, z: 8, core: 2. Of those that a mesh axis runs over, the one named last changes fastest.
Arguments:
- displacement: float32 [3, 128, 64, 256], P(None, 'pts', 'bond'), may hold values from -1.5 to 1.5
- velocity: float32 [3, 128, 64, 256], P(None, 'pts', 'bond'), may hold values from -6 to 6
- stiffness: float32 [128, 64, 256], P('pts', 'bond'), may hold values from 0.5 to 8
- offsets: int32 [256, 3], P('bond'), may hold values from -4 to 4, as said below
- intact: int32 [256, 128, 64, 256], P('bond', 'pts'), may hold values 0 or 1
Outputs:
- new_displacement: float32 [3, 128, 64, 256], P(None, 'pts', 'bond')
- new_velocity: float32 [3, 128, 64, 256], P(None, 'pts', 'bond')
The draws below stay inside these ranges and needn't reach their ends.
Inputs may be any that keep to these rules, and one draw needn't show every extreme that they name: `offsets`: every nonzero lattice shift (a, b, c) with a * a + b * b + c * c <= 16, each exactly once, in an order drawn from the seed.
All inputs are finite; a program needn't handle non-finite values. No bound on the sum of `intact` on one device may be relied on, other than what follows from the above.
Results may differ from the reference program's by a relative error of at most 0.0003.
Values sent between devices are 32-bit elements; how exact they have to be, the bound alone decides.
A program may use at most 64 MiB of HBM per device.

```python
import math
import jax
import jax.numpy as jnp
from jax import lax

REACH = 4
OFFSETS = 256
NY = 64
NZ = 256
NX = 128


def draw_offsets(key, part):
    side = 2 * REACH + 1
    shuffled = jax.random.permutation(key, side * side * side).astype(jnp.int32)
    first = shuffled // (side * side) - REACH
    second = shuffled // side % side - REACH
    third = shuffled % side - REACH
    radius = first * first + second * second + third * third
    outside = ((radius > REACH * REACH) | (radius == 0)).astype(jnp.int32)
    order = jnp.argsort(outside, stable=True)[:OFFSETS]
    return jnp.stack([first[order], second[order], third[order]], axis=1).astype(jnp.int32)


def touch_ends(entries, own_key, smallest, top_value):
    longest = entries.shape.index(max(entries.shape))
    spots = []
    for shift in (0, 1):
        where = [jax.random.randint(jax.random.fold_in(own_key, axis), (), 0, length) for axis, length in enumerate(entries.shape)]
        where[longest] = (where[longest] + shift) % entries.shape[longest]
        spots.append(tuple(where))
    return entries.at[spots[0]].set(smallest).at[spots[1]].set(top_value)


def level_of(key, shape, cuts, smallest, largest):
    factor_of, own = 1.0, jax.random.fold_in(key, 6)
    for axis_at, shards_of in cuts:
        heights = jnp.exp(jax.random.uniform(jax.random.fold_in(own, axis_at), (shards_of,), jnp.float32, smallest / len(cuts), largest / len(cuts)))
        factor_of = factor_of * jnp.repeat(heights, shape[axis_at] // shards_of).reshape([-1 if axis == axis_at else 1 for axis in range(len(shape))])
    return factor_of


def centred(own_key, extent, deviation, bound, cuts=(), kind=jnp.bfloat16):
    values = jax.random.normal(own_key, extent, jnp.float32) * deviation
    if len(cuts) > 0:
        values = level_of(own_key, extent, cuts, -0.22, 0.18) * values
    return jnp.clip(values, min=-bound, max=bound).astype(kind)


def setup_inputs(seed: int = 0) -> dict:
    splits = jax.random.split(jax.random.key(seed), 6)
    return {
        "displacement": centred(splits[0], (3, NX, NY, NZ), 0.5, 1.5, ((1, 32), (2, 8)), jnp.float32),
        "velocity": centred(splits[1], (3, NX, NY, NZ), 1.0, 6.0, ((1, 32), (2, 8)), jnp.float32),
        "stiffness": jnp.clip(jnp.exp(math.log(8.0) - 2.7725887 * jax.random.uniform(splits[2], (NX, NY, NZ), jnp.float32) ** level_of(splits[2], (NX, NY, NZ), ((0, 32), (1, 8)), -0.2, 0.2)), 0.5, 8.0),
        "offsets": draw_offsets(jax.random.fold_in(splits[5], 71), 0),
        "intact": touch_ends((jax.random.randint(splits[4], (OFFSETS, NX, NY, NZ), 0, 4) < 3).astype(jnp.int32), jax.random.fold_in(splits[4], 1), 0, 1),
    }


SPACING = 6.0
FORCE_SCALE = 8.0
TIME_STEP = 0.5

def bond_forces(centre, padded, inside, shift, alive):
    shape = centre.shape
    lower = (shift + REACH).astype(jnp.int32)
    anchor = jnp.zeros((), jnp.int32)
    nearby = lax.dynamic_slice(padded, (anchor, lower[0], lower[1], lower[2]), shape)
    present = lax.dynamic_slice(inside, (lower[0], lower[1], lower[2]), shape[1:]) * alive.astype(centre.dtype)
    bond_vec = shift.astype(centre.dtype) * SPACING
    length = jnp.sqrt(jnp.sum(bond_vec * bond_vec))
    relative = bond_vec[:, None, None, None] + nearby[:3] - centre[:3]
    stretched = jnp.sqrt(lax.optimization_barrier(jnp.sum(relative * relative, axis=0)))
    strain = (stretched - length) / length
    coupling = 0.5 * (centre[3] + nearby[3]) * present / length
    return relative * (coupling * strain / stretched)

def reference(displacement, velocity, stiffness, offsets, intact):
    centre = jnp.concatenate([displacement, stiffness[None]], axis=0)
    padded = jnp.pad(centre, ((0, 0), (REACH, REACH), (REACH, REACH), (REACH, REACH)))
    inside = jnp.pad(jnp.ones(stiffness.shape, jnp.float32), REACH)

    def accumulate(total, pieces):
        shift, alive = pieces
        return (total + bond_forces(centre, padded, inside, shift, alive), None)
    total = lax.scan(accumulate, jnp.zeros(displacement.shape, jnp.float32), (offsets, intact))[0]
    density = FORCE_SCALE * total
    new_velocity = velocity + TIME_STEP * density
    new_displacement = displacement + TIME_STEP * new_velocity
    return (new_displacement, new_velocity)
```

```python
import functools

import jax
import jax.numpy as jnp
from jax import lax
from jax.experimental import pallas as pl
from jax.experimental.pallas import tpu as pltpu
from jax.sharding import PartitionSpec as P

REACH = 4
SPACING = 6.0
FORCE_SCALE = 8.0
TIME_STEP = 0.5
SHIFTS = 2 * REACH + 1
LANES = 128
SUB = 8


def build_rows(table, load, slab, slab_rows, ytile, lane):
    for row in range(slab_rows):
        at = slab * slab_rows + row
        for comp in range(4):
            left, right = load(comp, row)
            if comp == 0:
                height = SPACING * (at - REACH - slab_rows // 2)
                left, right = left + height, right + height
            for shift in range(-REACH, REACH + 1):
                if shift == 0:
                    out = (left, right)
                elif shift > 0:
                    near = lane < LANES - shift
                    turned_l = pltpu.roll(left, LANES - shift, 1)
                    turned_r = pltpu.roll(right, LANES - shift, 1)
                    out = (jnp.where(near, turned_l, turned_r), jnp.where(near, turned_r, 0.0))
                else:
                    near = lane < -shift
                    turned_l = pltpu.roll(left, -shift, 1)
                    turned_r = pltpu.roll(right, -shift, 1)
                    out = (jnp.where(near, 0.0, turned_l), jnp.where(near, turned_l, turned_r))
                if comp == 2:
                    out = (out[0] + SPACING * shift, out[1] + SPACING * shift)
                base = ((shift + REACH) * 3 * slab_rows + at) * 2
                rows = pl.ds(pl.multiple_of(SUB + ytile * SUB, SUB), SUB)
                for half in range(2):
                    table[comp, base + half, rows, :] = out[half]


def clear_edges(table, slab_rows, ytiles):
    zero = jnp.zeros((SUB, LANES), jnp.float32)

    def body(index, carry):
        for comp in range(4):
            table[comp, index, pl.ds(0, SUB), :] = zero
            table[comp, index, pl.ds(SUB * (ytiles + 1), SUB), :] = zero
        return carry

    lax.fori_loop(0, SHIFTS * 3 * slab_rows * 2, body, 0)


def build_inside(inside, ytiles, lane):
    zero = jnp.zeros((SUB, LANES), jnp.float32)
    one = jnp.ones((SUB, LANES), jnp.float32)
    for index in range(SHIFTS + 1):
        shift = index - REACH
        for half in range(2):
            mask = zero
            if index < SHIFTS:
                z = lane + half * LANES + shift
                mask = jnp.where((z >= 0) & (z < 2 * LANES), one, zero)
            for tile in range(ytiles + 2):
                inner = 0 < tile <= ytiles
                inside[index, half, pl.ds(tile * SUB, SUB), :] = mask if inner else zero


def build_constants(constants, offsets):
    scale = FORCE_SCALE * TIME_STEP * 0.5
    zero = jnp.zeros((SUB, LANES), jnp.float32)

    def body(k, carry):
        a, b, c = offsets[k, 0], offsets[k, 1], offsets[k, 2]
        square = zero + (SPACING * SPACING) * (a * a + b * b + c * c).astype(jnp.float32)
        constants[k, 0] = scale / square
        constants[k, 1] = scale / jnp.sqrt(square)
        return carry

    lax.fori_loop(0, offsets.shape[0], body, 0)


def tile_force(table, inside, constants, offsets, alive, ytile, half, slab_rows, total_rows, first):
    count = offsets.shape[0]
    middle = SHIFTS // 2 * 3 * slab_rows
    here = pl.ds(pl.multiple_of(SUB + ytile * SUB, SUB), SUB)
    centre = [
        [table[comp, (middle + slab_rows + row) * 2 + half, here, :] for comp in range(4)]
        for row in range(slab_rows)
    ]

    def body(k, total):
        a, b, c = offsets[k, 0], offsets[k, 1], offsets[k, 2]
        start = ((c + REACH) * 3 * slab_rows + slab_rows + a) * 2 + half
        rows = pl.ds(SUB + ytile * SUB + b, SUB)
        rise = SPACING * b.astype(jnp.float32)
        c0, c1 = constants[k, 0], constants[k, 1]
        out = []
        for row in range(slab_rows):
            at = first + row + a
            valid = (at >= 0) & (at < total_rows)
            present = inside[jnp.where(valid, c + REACH, SHIFTS), half, rows, :]
            x, y, z, micro = (table[comp, start + 2 * row, rows, :] for comp in range(4))
            px, py, pz, pmicro = centre[row]
            rx = x - px
            ry = (y + rise) - py
            rz = z - pz
            inverse = lax.rsqrt(rx * rx + ry * ry + rz * rz)
            mask = alive(k, row, half).astype(jnp.float32)
            weight = (pmicro * present + micro) * mask * (c0 - c1 * inverse)
            fx, fy, fz = total[row]
            out.append((fx + weight * rx, fy + weight * ry, fz + weight * rz))
        return tuple(out)

    zero = jnp.zeros((SUB, LANES), jnp.float32)
    start_total = tuple((zero, zero, zero) for _ in range(slab_rows))
    return lax.fori_loop(0, count, body, start_total, unroll=2)


def force_kernel(
    pts, slab_rows, ytiles, offsets, low, mid, high, intact, out, table, inside, constants, mask, sem
):
    def fetch(tile):
        return pltpu.make_async_copy(
            intact.at[:, :, pl.ds(tile * SUB, SUB), :], mask.at[tile], sem.at[tile]
        )

    for tile in range(ytiles):
        fetch(tile).start()
    lane = lax.broadcasted_iota(jnp.int32, (SUB, LANES), 1)
    build_constants(constants, offsets)
    build_inside(inside, ytiles, lane)
    clear_edges(table, slab_rows, ytiles)

    def build(tile, carry):
        for slab, source in enumerate((low, mid, high)):

            def load(comp, row, source=source):
                return (
                    source[tile, comp, row, :, pl.ds(0, LANES)],
                    source[tile, comp, row, :, pl.ds(LANES, LANES)],
                )

            build_rows(table, load, slab, slab_rows, tile, lane)
        return carry

    lax.fori_loop(0, ytiles, build, 0)
    first = lax.axis_index("pts") * slab_rows

    def work(tile, carry):
        fetch(tile).wait()
        for half in range(2):

            def alive(k, row, half):
                return mask[tile, k, row, :, pl.ds(half * LANES, LANES)]

            total = tile_force(
                table, inside, constants, offsets, alive, tile, half,
                slab_rows, slab_rows * pts, first,
            )
            for row in range(slab_rows):
                for comp in range(3):
                    out[tile, comp, row, :, pl.ds(half * LANES, LANES)] = total[row][comp]
        return carry

    lax.fori_loop(0, ytiles, work, 0)


def on_device(pts, displacement, velocity, stiffness, offsets, intact):
    slab_rows = displacement.shape[1]
    count, _, ny, nz = intact.shape
    ytiles = ny // SUB
    own = jnp.concatenate([displacement, stiffness[None]], axis=0)
    copies = jnp.broadcast_to(own, (ytiles, *own.shape))
    mid = lax.all_to_all(copies, "bond", split_axis=0, concat_axis=0, tiled=True)
    up = [(i, i + 1) for i in range(pts - 1)]
    low = lax.ppermute(mid, "pts", up)
    high = lax.ppermute(mid, "pts", [(j, i) for i, j in up])
    vmem = pl.BlockSpec(memory_space=pltpu.VMEM)
    force = pl.pallas_call(
        functools.partial(force_kernel, pts, slab_rows, ytiles),
        out_shape=jax.ShapeDtypeStruct((ytiles, 3, slab_rows, SUB, nz), jnp.float32),
        in_specs=[
            pl.BlockSpec(memory_space=pltpu.SMEM), vmem, vmem, vmem,
            pl.BlockSpec(memory_space=pl.ANY),
        ],
        out_specs=vmem,
        scratch_shapes=[
            pltpu.VMEM((4, SHIFTS * 3 * slab_rows * 2, (ytiles + 2) * SUB, LANES), jnp.float32),
            pltpu.VMEM((SHIFTS + 1, 2, (ytiles + 2) * SUB, LANES), jnp.float32),
            pltpu.VMEM((count, 2, SUB, LANES), jnp.float32),
            pltpu.VMEM((ytiles, count, slab_rows, SUB, nz), jnp.int32),
            pltpu.SemaphoreType.DMA((ytiles,)),
        ],
        compiler_params=pltpu.CompilerParams(vmem_limit_bytes=60 << 20),
        name="bond_forces",
    )(offsets, low, mid, high, intact)
    arrived = lax.all_to_all(force, "bond", split_axis=0, concat_axis=0, tiled=True)
    new_velocity = velocity + arrived.sum(axis=0)
    new_displacement = displacement + TIME_STEP * new_velocity
    return new_displacement, new_velocity


def solution(mesh):
    return jax.shard_map(
        functools.partial(on_device, mesh.shape["pts"]),
        mesh=mesh,
        in_specs=(
            P(None, "pts", "bond", None),
            P(None, "pts", "bond", None),
            P("pts", "bond", None),
            P("bond", None),
            P("bond", "pts", None, None),
        ),
        out_specs=(P(None, "pts", "bond", None), P(None, "pts", "bond", None)),
        check_vma=False,
    )
```

```python
import functools

import jax
import jax.numpy as jnp
from jax import lax
from jax.experimental import pallas as pl
from jax.experimental.pallas import tpu as pltpu
from jax.sharding import PartitionSpec as P

REACH = 4
SPACING = 6.0
FORCE_SCALE = 8.0
TIME_STEP = 0.5
SHIFTS = 2 * REACH + 1
LANES = 128
SUB = 8
RING = 4
MESH = pl.DeviceIdType.MESH


def needed_rows(slab, shift, rows):
    if slab == 1:
        return 0, rows
    depth = max(d for d in range(rows + 1) if d * d + shift * shift <= REACH * REACH)
    return (rows - depth, rows) if slab == 0 else (0, depth)


def build_piece(table, pieces, slab, ytile, rows, lane):
    here = pl.ds(pl.multiple_of(SUB + ytile * SUB, SUB), SUB)
    for comp in range(4):
        left = pieces[slab, ytile, comp, :, :, pl.ds(0, LANES)]
        right = pieces[slab, ytile, comp, :, :, pl.ds(LANES, LANES)]
        if comp == 0:
            step = lax.broadcasted_iota(jnp.int32, left.shape, 0).astype(jnp.float32)
            height = SPACING * (step + float((slab - 1) * rows - rows // 2))
            left, right = left + height, right + height
        for shift in range(-REACH, REACH + 1):
            lo, hi = needed_rows(slab, shift, rows)
            if hi == lo:
                continue
            l, r = left[lo:hi], right[lo:hi]
            near = lane[lo:hi]
            if shift == 0:
                out = (l, r)
            elif shift > 0:
                near = near < LANES - shift
                l = pltpu.roll(l, LANES - shift, 2)
                r = pltpu.roll(r, LANES - shift, 2)
                out = (jnp.where(near, l, r), jnp.where(near, r, 0.0))
            else:
                near = near < -shift
                l = pltpu.roll(l, -shift, 2)
                r = pltpu.roll(r, -shift, 2)
                out = (jnp.where(near, 0.0, l), jnp.where(near, l, r))
            if comp == 2:
                out = (out[0] + SPACING * shift, out[1] + SPACING * shift)
            for half in range(2):
                at = (shift + REACH) * 2 + half
                table[comp, at, pl.ds(slab * rows + lo, hi - lo), here, :] = out[half]


def build_frame(table, rows, ytiles, first, total_rows):
    shape = (3 * rows, SUB, LANES)
    zero = jnp.zeros(shape, jnp.float32)
    lane = lax.broadcasted_iota(jnp.int32, shape, 2)
    row = lax.broadcasted_iota(jnp.int32, shape, 0) + (first - rows)
    row_in = (row >= 0) & (row < total_rows)

    def body(at, carry):
        z = lane + at % 2 * LANES + (at // 2 - REACH)
        mask = jnp.where(row_in & (z >= 0) & (z < 2 * LANES), 1.0, 0.0)
        for comp in range(5):
            table[comp, at, :, pl.ds(0, SUB), :] = zero
            table[comp, at, :, pl.ds(SUB * (ytiles + 1), SUB), :] = zero
        for tile in range(ytiles):
            table[4, at, :, pl.ds(SUB * (tile + 1), SUB), :] = mask
        return carry

    lax.fori_loop(0, 2 * SHIFTS, body, 0)


def build_constants(constants, offsets, count):
    scale = FORCE_SCALE * TIME_STEP * 0.5
    zero = jnp.zeros((SUB, LANES), jnp.float32)

    def body(k, carry):
        a, b, c = offsets[0, k], offsets[1, k], offsets[2, k]
        square = zero + (SPACING * SPACING) * (a * a + b * b + c * c).astype(jnp.float32)
        constants[k, 0] = scale / square
        constants[k, 1] = scale / jnp.sqrt(square)
        constants[k, 2] = zero + SPACING * b.astype(jnp.float32)
        return carry

    lax.fori_loop(0, count, body, 0)


def tile_force(table, constants, offsets, mask, ytile, half, rows, count):
    here = pl.ds(pl.multiple_of(SUB + ytile * SUB, SUB), SUB)
    px, py, pz, pmicro = (
        table[comp, REACH * 2 + half, pl.ds(rows, rows), here, :] for comp in range(4)
    )

    def body(k, total):
        a, b, c = offsets[0, k], offsets[1, k], offsets[2, k]
        at = (c + REACH) * 2 + half
        slab = pl.ds(rows + a, rows)
        there = pl.ds(SUB + ytile * SUB + b, SUB)
        x, y, z, micro, inside = (table[comp, at, slab, there, :] for comp in range(5))
        rx = x - px
        ry = (y + constants[k, 2]) - py
        rz = z - pz
        inverse = lax.rsqrt(rx * rx + ry * ry + rz * rz)
        alive = mask[ytile, k, :, :, pl.ds(half * LANES, LANES)].astype(jnp.float32)
        weight = (pmicro * inside + micro) * alive * (constants[k, 0] - constants[k, 1] * inverse)
        fx, fy, fz = total
        return fx + weight * rx, fy + weight * ry, fz + weight * rz

    zero = jnp.zeros((rows, SUB, LANES), jnp.float32)
    return lax.fori_loop(0, count, body, (zero, zero, zero), unroll=4)


def step_kernel(
    pts, rows, ytiles, count,
    offsets, displacement, stiffness, intact, out,
    table, constants, pieces, mask, partial, arrived,
    load_sem, mask_sem, send_sem, mid_sem, near_sem, far_sem, back_send, back_sem,
):
    p, b = lax.axis_index("pts"), lax.axis_index("bond")
    pair, y = b // RING, b % RING
    core = p % 2
    near_p = p + 1 - 2 * core
    far_p = p - 1 + 2 * core
    has_far = (far_p >= 0) & (far_p < pts)
    near_slot, far_slot = 2 - 2 * core, 2 * core

    def place(flip, turn):
        return (pair + flip) % 2 * RING + (y + turn) % RING

    def fetch(tile):
        return pltpu.make_async_copy(
            intact.at[:, :, pl.ds(tile * SUB, SUB), :], mask.at[tile], mask_sem.at[tile]
        )

    loads = [
        pltpu.make_async_copy(displacement, pieces.at[1, b, pl.ds(0, 3)], load_sem.at[0]),
        pltpu.make_async_copy(stiffness, pieces.at[1, b, 3], load_sem.at[1]),
    ]
    for load in loads:
        load.start()
    barrier = pltpu.get_barrier_semaphore()
    for other in range(1, 2 * RING):
        pl.semaphore_signal(
            barrier, inc=1, device_id=(p, place(other // RING, other % RING)), device_id_type=MESH
        )
    pl.semaphore_signal(barrier, inc=1, device_id=(near_p, b), device_id_type=MESH)

    @pl.when(has_far)
    def _():
        pl.semaphore_signal(
            barrier, inc=1, device_id=(far_p, place(1, 0)), device_id_type=MESH
        )

    @pl.when(has_far)
    def _():
        pl.semaphore_wait(barrier, 2 * RING + 1)

    @pl.when(jnp.logical_not(has_far))
    def _():
        pl.semaphore_wait(barrier, 2 * RING)

    for load in loads:
        load.wait()

    used = []

    def copy_of(source_slot, slot, origin, device, sems):
        index = len(used)
        return pltpu.make_async_remote_copy(
            src_ref=pieces.at[source_slot, origin],
            dst_ref=pieces.at[slot, origin],
            send_sem=send_sem.at[index],
            recv_sem=sems.at[origin],
            device_id=device,
            device_id_type=MESH,
        )

    def along(origin, flip, turn):
        copy = copy_of(1, 1, origin, (p, place(flip, turn)), mid_sem)
        used.append((copy, False))
        copy.start()

    def to_near(origin):
        copy = copy_of(1, far_slot, origin, (near_p, b), near_sem)
        used.append((copy, False))
        copy.start()

    def to_far(origin):
        copy = copy_of(1, near_slot, origin, (far_p, place(1, 0)), far_sem)
        used.append((copy, True))

        @pl.when(has_far)
        def _():
            copy.start()

    def far_on(origin):
        copy = copy_of(far_slot, far_slot, origin, (p, place(1, 0)), far_sem)
        used.append((copy, True))

        @pl.when(has_far)
        def _():
            arrival(far_slot, origin, far_sem).wait_recv()
            copy.start()

    def arrival(slot, origin, sems):
        return pltpu.make_async_remote_copy(
            src_ref=pieces.at[slot, origin],
            dst_ref=pieces.at[slot, origin],
            send_sem=send_sem.at[0],
            recv_sem=sems.at[origin],
            device_id=(near_p, b),
            device_id_type=MESH,
        )

    def await_mid(flip, turn):
        origin = place(flip, turn)
        arrival(1, origin, mid_sem).wait_recv()
        return origin

    lane = lax.broadcasted_iota(jnp.int32, (rows, SUB, LANES), 2)

    def build(slab, tiles):
        build_piece(table, pieces, slab, tiles, rows, lane)

    own = place(0, 0)
    along(own, 0, 1)
    to_far(own)
    along(own, 1, 0)
    along(own, 0, -1)
    to_near(own)
    for tile in range(ytiles):
        fetch((b + 1 + tile) % ytiles).start()
    build_constants(constants, offsets, count)
    build_frame(table, rows, ytiles, p * rows, pts * rows)

    @pl.when(jnp.logical_not(has_far))
    def _():
        def clear(tile, carry):
            pieces[far_slot, tile] = jnp.zeros(pieces.shape[2:], jnp.float32)
            return carry

        lax.fori_loop(0, ytiles, clear, 0)

    origin = await_mid(0, -1)
    to_far(origin)
    along(origin, 0, 1)
    to_near(origin)
    origin = await_mid(0, 1)
    to_far(origin)
    to_near(origin)
    origin = await_mid(1, 0)
    along(origin, 0, -1)
    along(origin, 0, 1)
    to_near(origin)
    far_on(place(1, 0))

    def build_mid(flip, start, number):
        def body(index, carry):
            build(1, place(flip, start + index))
            return carry

        lax.fori_loop(0, number, body, 0)

    def build_side(lower, origin):
        @pl.when(lower)
        def _():
            build(0, origin)

        @pl.when(jnp.logical_not(lower))
        def _():
            build(2, origin)

    def build_near(flip, start, number):
        def body(index, carry):
            origin = place(flip, start + index)
            arrival(near_slot, origin, near_sem).wait_recv()
            build_side(core == 1, origin)
            return carry

        lax.fori_loop(0, number, body, 0)

    def build_far(flip, start, number, waited):
        def body(index, carry):
            origin = place(flip, start + index)
            if not waited:

                @pl.when(has_far)
                def _():
                    arrival(far_slot, origin, far_sem).wait_recv()

            build_side(core == 0, origin)
            return carry

        lax.fori_loop(0, number, body, 0)

    build_mid(0, -1, 3)
    build_near(0, -1, 3)
    far_on(place(1, -1))
    far_on(place(1, 1))
    origin = await_mid(0, 2)
    to_far(origin)
    to_near(origin)
    origin = await_mid(1, 1)
    along(origin, 0, -1)
    to_near(origin)
    origin = await_mid(1, -1)
    to_near(origin)
    build_mid(0, 2, 1)
    build_mid(1, -1, 3)
    build_far(1, -1, 3, True)
    origin = await_mid(1, 2)
    to_near(origin)
    far_on(place(1, 2))
    build_near(1, -1, 3)
    build_near(0, 2, 1)
    build_mid(1, 2, 1)
    build_far(1, 2, 1, True)
    build_near(1, 2, 1)
    build_far(0, -1, 4, False)

    def back(step, tile):
        return pltpu.make_async_remote_copy(
            src_ref=partial.at[tile],
            dst_ref=arrived.at[step],
            send_sem=back_send.at[step],
            recv_sem=back_sem.at[step],
            device_id=(p, tile),
            device_id_type=MESH,
        )

    def target(step):
        return place(1 - step // RING, step + 1)

    def work(step, carry):
        tile = target(step)
        fetch(tile).wait()
        for half in range(2):
            total = tile_force(table, constants, offsets, mask, tile, half, rows, count)
            for comp in range(3):
                partial[tile, comp, :, :, pl.ds(half * LANES, LANES)] = total[comp]
            if half == 0:

                @pl.when(step > 0)
                def _():
                    back(step - 1, target(step - 1)).start()

        return carry

    lax.fori_loop(0, ytiles, work, 0)
    for copy, far in used:
        if far:

            @pl.when(has_far)
            def _(copy=copy):
                copy.wait_send()
        else:
            copy.wait_send()
    total = partial[b]
    for step in range(ytiles - 1):
        back(step, target(step)).wait_send()
        back(step, target(step)).wait_recv()
        total = total + arrived[step]
    out[...] = total


def on_device(pts, displacement, velocity, stiffness, offsets, intact):
    rows = displacement.shape[1]
    count, _, ny, nz = intact.shape
    ytiles = ny // SUB
    anywhere = pl.BlockSpec(memory_space=pl.ANY)
    change = pl.pallas_call(
        functools.partial(step_kernel, pts, rows, ytiles, count),
        out_shape=jax.ShapeDtypeStruct((3, rows, SUB, nz), jnp.float32),
        in_specs=[pl.BlockSpec(memory_space=pltpu.SMEM), anywhere, anywhere, anywhere],
        out_specs=pl.BlockSpec(memory_space=pltpu.VMEM),
        scratch_shapes=[
            pltpu.VMEM((5, SHIFTS * 2, 3 * rows, (ytiles + 2) * SUB, LANES), jnp.float32),
            pltpu.VMEM((count, 3, SUB, LANES), jnp.float32),
            pltpu.VMEM((3, ytiles, 4, rows, SUB, nz), jnp.float32),
            pltpu.VMEM((ytiles, count, rows, SUB, nz), jnp.int32),
            pltpu.VMEM((ytiles, 3, rows, SUB, nz), jnp.float32),
            pltpu.VMEM((ytiles - 1, 3, rows, SUB, nz), jnp.float32),
            pltpu.SemaphoreType.DMA((2,)),
            pltpu.SemaphoreType.DMA((ytiles,)),
            pltpu.SemaphoreType.DMA((24,)),
            pltpu.SemaphoreType.DMA((ytiles,)),
            pltpu.SemaphoreType.DMA((ytiles,)),
            pltpu.SemaphoreType.DMA((ytiles,)),
            pltpu.SemaphoreType.DMA((ytiles,)),
            pltpu.SemaphoreType.DMA((ytiles,)),
        ],
        compiler_params=pltpu.CompilerParams(
            vmem_limit_bytes=67043328, collective_id=0, has_side_effects=True
        ),
        name="bond_step",
    )(offsets.T, displacement, stiffness, intact)
    new_velocity = velocity + change
    new_displacement = displacement + TIME_STEP * new_velocity
    return new_displacement, new_velocity


def solution(mesh):
    return jax.shard_map(
        functools.partial(on_device, mesh.shape["pts"]),
        mesh=mesh,
        in_specs=(
            P(None, "pts", "bond", None),
            P(None, "pts", "bond", None),
            P("pts", "bond", None),
            P("bond", None),
            P("bond", "pts", None, None),
        ),
        out_specs=(P(None, "pts", "bond", None), P(None, "pts", "bond", None)),
        check_vma=False,
    )
```

```python
import functools

import jax
import jax.numpy as jnp
from jax import lax
from jax.experimental import pallas as pl
from jax.experimental.pallas import tpu as pltpu
from jax.sharding import PartitionSpec as P

REACH = 4
SPACING = 6.0
FORCE_SCALE = 8.0
TIME_STEP = 0.5
SHIFTS = 2 * REACH + 1
LANES = 128
SUB = 8
RING = 4
MESH = pl.DeviceIdType.MESH


def needed_rows(slab, shift, rows):
    if slab == 1:
        return 0, rows
    depth = max(d for d in range(rows + 1) if d * d + shift * shift <= REACH * REACH)
    return (rows - depth, rows) if slab == 0 else (0, depth)


def build_piece(table, pieces, slab, ytile, rows, lane):
    here = pl.ds(pl.multiple_of(SUB + ytile * SUB, SUB), SUB)
    for comp in range(4):
        left = pieces[slab, ytile, comp, :, :, pl.ds(0, LANES)]
        right = pieces[slab, ytile, comp, :, :, pl.ds(LANES, LANES)]
        if comp == 0:
            step = lax.broadcasted_iota(jnp.int32, left.shape, 0).astype(jnp.float32)
            height = SPACING * (step + float((slab - 1) * rows - rows // 2))
            left, right = left + height, right + height
        for shift in range(-REACH, REACH + 1):
            lo, hi = needed_rows(slab, shift, rows)
            if hi == lo:
                continue
            l, r = left[lo:hi], right[lo:hi]
            near = lane[lo:hi]
            if shift == 0:
                out = (l, r)
            elif shift > 0:
                near = near < LANES - shift
                l = pltpu.roll(l, LANES - shift, 2)
                r = pltpu.roll(r, LANES - shift, 2)
                out = (jnp.where(near, l, r), jnp.where(near, r, 0.0))
            else:
                near = near < -shift
                l = pltpu.roll(l, -shift, 2)
                r = pltpu.roll(r, -shift, 2)
                out = (jnp.where(near, 0.0, l), jnp.where(near, l, r))
            if comp == 2:
                out = (out[0] + SPACING * shift, out[1] + SPACING * shift)
            for half in range(2):
                at = (shift + REACH) * 2 + half
                table[comp, at, pl.ds(slab * rows + lo, hi - lo), here, :] = out[half]


def build_frame(table, rows, ytiles, first, total_rows):
    shape = (3 * rows, SUB, LANES)
    zero = jnp.zeros(shape, jnp.float32)
    lane = lax.broadcasted_iota(jnp.int32, shape, 2)
    row = lax.broadcasted_iota(jnp.int32, shape, 0) + (first - rows)
    row_in = (row >= 0) & (row < total_rows)

    def body(at, carry):
        z = lane + at % 2 * LANES + (at // 2 - REACH)
        mask = jnp.where(row_in & (z >= 0) & (z < 2 * LANES), 1.0, 0.0)
        for comp in range(5):
            table[comp, at, :, pl.ds(0, SUB), :] = zero
            table[comp, at, :, pl.ds(SUB * (ytiles + 1), SUB), :] = zero
        for tile in range(ytiles):
            table[4, at, :, pl.ds(SUB * (tile + 1), SUB), :] = mask
        return carry

    lax.fori_loop(0, 2 * SHIFTS, body, 0)


def build_constants(constants, offsets, count):
    scale = FORCE_SCALE * TIME_STEP * 0.5
    zero = jnp.zeros((SUB, LANES), jnp.float32)

    def body(k, carry):
        a, b, c = offsets[0, k], offsets[1, k], offsets[2, k]
        square = zero + (SPACING * SPACING) * (a * a + b * b + c * c).astype(jnp.float32)
        constants[k, 0] = scale / square
        constants[k, 1] = scale / jnp.sqrt(square)
        constants[k, 2] = zero + SPACING * b.astype(jnp.float32)
        return carry

    lax.fori_loop(0, count, body, 0)


def tile_force(table, constants, offsets, mask, ytile, half, rows, count):
    here = pl.ds(pl.multiple_of(SUB + ytile * SUB, SUB), SUB)
    px, py, pz, pmicro = (
        table[comp, REACH * 2 + half, pl.ds(rows, rows), here, :] for comp in range(4)
    )

    def body(k, total):
        a, b, c = offsets[0, k], offsets[1, k], offsets[2, k]
        at = (c + REACH) * 2 + half
        slab = pl.ds(rows + a, rows)
        there = pl.ds(SUB + ytile * SUB + b, SUB)
        x, y, z, micro, inside = (table[comp, at, slab, there, :] for comp in range(5))
        rx = x - px
        ry = (y + constants[k, 2]) - py
        rz = z - pz
        inverse = lax.rsqrt(rx * rx + ry * ry + rz * rz)
        alive = mask[ytile, k, :, :, pl.ds(half * LANES, LANES)].astype(jnp.float32)
        weight = (pmicro * inside + micro) * alive * (constants[k, 0] - constants[k, 1] * inverse)
        fx, fy, fz = total
        return fx + weight * rx, fy + weight * ry, fz + weight * rz

    zero = jnp.zeros((rows, SUB, LANES), jnp.float32)
    return lax.fori_loop(0, count, body, (zero, zero, zero), unroll=4)


def step_kernel(
    pts, rows, ytiles, count,
    offsets, displacement, stiffness, intact, out,
    table, constants, pieces, mask, partial, arrived,
    load_sem, mask_sem, send_sem, mid_sem, near_sem, far_sem, back_send, back_sem,
):
    p, b = lax.axis_index("pts"), lax.axis_index("bond")
    pair, y = b // RING, b % RING
    core = p % 2
    near_p = p + 1 - 2 * core
    far_p = p - 1 + 2 * core
    has_far = (far_p >= 0) & (far_p < pts)
    near_slot, far_slot = 2 - 2 * core, 2 * core

    def place(flip, turn):
        return (pair + flip) % 2 * RING + (y + turn) % RING

    def fetch(tile):
        return pltpu.make_async_copy(
            intact.at[:, :, pl.ds(tile * SUB, SUB), :], mask.at[tile], mask_sem.at[tile]
        )

    loads = [
        pltpu.make_async_copy(displacement, pieces.at[1, b, pl.ds(0, 3)], load_sem.at[0]),
        pltpu.make_async_copy(stiffness, pieces.at[1, b, 3], load_sem.at[1]),
    ]
    for load in loads:
        load.start()
    barrier = pltpu.get_barrier_semaphore()
    for other in range(1, 2 * RING):
        pl.semaphore_signal(
            barrier, inc=1, device_id=(p, place(other // RING, other % RING)), device_id_type=MESH
        )
    pl.semaphore_signal(barrier, inc=1, device_id=(near_p, b), device_id_type=MESH)

    @pl.when(has_far)
    def _():
        pl.semaphore_signal(
            barrier, inc=1, device_id=(far_p, place(1, 0)), device_id_type=MESH
        )

    @pl.when(has_far)
    def _():
        pl.semaphore_wait(barrier, 2 * RING + 1)

    @pl.when(jnp.logical_not(has_far))
    def _():
        pl.semaphore_wait(barrier, 2 * RING)

    for load in loads:
        load.wait()

    used = []

    def copy_of(source_slot, slot, origin, comps, device, sem):
        copy = pltpu.make_async_remote_copy(
            src_ref=pieces.at[source_slot, origin, comps],
            dst_ref=pieces.at[slot, origin, comps],
            send_sem=send_sem.at[len(used)],
            recv_sem=sem,
            device_id=device,
            device_id_type=MESH,
        )
        return copy

    def comps_of(part):
        return pl.ds(2 * part, 2)

    def along(origin, part, flip, turn):
        copy = copy_of(
            1, 1, origin, comps_of(part), (p, place(flip, turn)), mid_sem.at[origin, part]
        )
        used.append((copy, False))
        copy.start()

    def to_near(origin):
        copy = copy_of(1, far_slot, origin, pl.ds(0, 4), (near_p, b), near_sem.at[origin])
        used.append((copy, False))
        copy.start()

    def to_far(origin, part):
        copy = copy_of(
            1, near_slot, origin, comps_of(part), (far_p, place(1, 0)), far_sem.at[origin, part]
        )
        used.append((copy, True))

        @pl.when(has_far)
        def _():
            copy.start()

    def far_on(origin, part):
        copy = copy_of(
            far_slot, far_slot, origin, comps_of(part), (p, place(1, 0)), far_sem.at[origin, part]
        )
        used.append((copy, True))

        @pl.when(has_far)
        def _():
            arrival(far_slot, origin, comps_of(part), far_sem.at[origin, part]).wait_recv()
            copy.start()

    def arrival(slot, origin, comps, sem):
        return pltpu.make_async_remote_copy(
            src_ref=pieces.at[slot, origin, comps],
            dst_ref=pieces.at[slot, origin, comps],
            send_sem=send_sem.at[0],
            recv_sem=sem,
            device_id=(near_p, b),
            device_id_type=MESH,
        )

    def await_mid(flip, turn, part):
        origin = place(flip, turn)
        arrival(1, origin, comps_of(part), mid_sem.at[origin, part]).wait_recv()
        return origin

    lane = lax.broadcasted_iota(jnp.int32, (rows, SUB, LANES), 2)

    def build(slab, tiles):
        build_piece(table, pieces, slab, tiles, rows, lane)

    own = place(0, 0)
    for part in range(2):
        along(own, part, 0, 1)
        along(own, part, 0, -1)
        to_far(own, part)
        along(own, part, 1, 0)
    to_near(own)
    for tile in range(ytiles):
        fetch((b + 1 + tile) % ytiles).start()
    build_constants(constants, offsets, count)
    build_frame(table, rows, ytiles, p * rows, pts * rows)

    @pl.when(jnp.logical_not(has_far))
    def _():
        def clear(tile, carry):
            pieces[far_slot, tile] = jnp.zeros(pieces.shape[2:], jnp.float32)
            return carry

        lax.fori_loop(0, ytiles, clear, 0)

    for part in range(2):
        origin = await_mid(0, -1, part)
        along(origin, part, 0, 1)
        to_far(origin, part)
        origin = await_mid(0, 1, part)
        to_far(origin, part)
        origin = await_mid(1, 0, part)
        along(origin, part, 0, -1)
        along(origin, part, 0, 1)
    for origin in (place(0, -1), place(0, 1), place(1, 0)):
        to_near(origin)
    for part in range(2):
        far_on(place(1, 0), part)

    def build_mid(flip, start, number):
        def body(index, carry):
            build(1, place(flip, start + index))
            return carry

        lax.fori_loop(0, number, body, 0)

    def build_side(lower, origin):
        @pl.when(lower)
        def _():
            build(0, origin)

        @pl.when(jnp.logical_not(lower))
        def _():
            build(2, origin)

    def build_near(flip, start, number):
        def body(index, carry):
            origin = place(flip, start + index)
            arrival(near_slot, origin, pl.ds(0, 4), near_sem.at[origin]).wait_recv()
            build_side(core == 1, origin)
            return carry

        lax.fori_loop(0, number, body, 0)

    def build_far(flip, start, number, waited):
        def body(index, carry):
            origin = place(flip, start + index)
            if not waited:

                @pl.when(has_far)
                def _():
                    for part in range(2):
                        arrival(
                            far_slot, origin, comps_of(part), far_sem.at[origin, part]
                        ).wait_recv()

            build_side(core == 0, origin)
            return carry

        lax.fori_loop(0, number, body, 0)

    build_mid(0, -1, 3)
    build_near(0, -1, 3)
    for part in range(2):
        origin = await_mid(0, 2, part)
        to_far(origin, part)
        far_on(place(1, -1), part)
    to_near(place(0, 2))
    for part in range(2):
        origin = await_mid(1, 1, part)
        along(origin, part, 0, -1)
    to_near(place(1, 1))
    for part in range(2):
        await_mid(1, -1, part)
    to_near(place(1, -1))
    for part in range(2):
        far_on(place(1, 1), part)
    build_mid(0, 2, 1)
    build_mid(1, -1, 3)
    build_far(1, -1, 3, True)
    build_near(1, -1, 3)
    build_near(0, 2, 1)
    for part in range(2):
        await_mid(1, 2, part)
    to_near(place(1, 2))
    for part in range(2):
        far_on(place(1, 2), part)
    build_mid(1, 2, 1)
    build_far(1, 2, 1, True)
    build_near(1, 2, 1)

    def back(step, slot, tile):
        return pltpu.make_async_remote_copy(
            src_ref=partial.at[tile],
            dst_ref=arrived.at[slot],
            send_sem=back_send.at[step],
            recv_sem=back_sem.at[slot],
            device_id=(p, tile),
            device_id_type=MESH,
        )

    across = 1 - pair
    last = 2 * RING - 1

    def early(step):
        return across * last + (1 - 2 * across) * ((step + y) % (RING - 1))

    border = RING - 1 + across

    def work(tile, between):
        fetch(tile).wait()
        for half in range(2):
            total = tile_force(table, constants, offsets, mask, tile, half, rows, count)
            for comp in range(3):
                partial[tile, comp, :, :, pl.ds(half * LANES, LANES)] = total[comp]
            if half == 0:
                between()

    def work_early(step, carry):
        def between():
            @pl.when(step > 0)
            def _():
                back(step - 1, y, early(step - 1)).start()

        work(early(step), between)
        return carry

    def work_late(step, carry):
        def between():
            @pl.when(step == RING)
            def _():
                back(RING - 1, y, border).start()

            @pl.when(step > RING)
            def _():
                back(step - 1, step - 1, place(0, step)).start()

        work(place(0, step + 1), between)
        return carry

    lax.fori_loop(0, RING - 1, work_early, 0)
    build_far(0, -1, 1, False)
    back(RING - 2, y, early(RING - 2)).start()
    build_far(0, 0, 3, False)
    work(border, lambda: None)
    lax.fori_loop(RING, 2 * RING, work_late, 0)
    for copy, far in used:
        if far:

            @pl.when(has_far)
            def _(copy=copy):
                copy.wait_send()
        else:
            copy.wait_send()
    total = partial[b]
    for slot in range(ytiles - 1):
        back(slot, slot, border).wait_send()
        back(slot, slot, border).wait_recv()
        total = total + arrived[slot]
    out[...] = total


def on_device(pts, displacement, velocity, stiffness, offsets, intact):
    rows = displacement.shape[1]
    count, _, ny, nz = intact.shape
    ytiles = ny // SUB
    anywhere = pl.BlockSpec(memory_space=pl.ANY)
    change = pl.pallas_call(
        functools.partial(step_kernel, pts, rows, ytiles, count),
        out_shape=jax.ShapeDtypeStruct((3, rows, SUB, nz), jnp.float32),
        in_specs=[pl.BlockSpec(memory_space=pltpu.SMEM), anywhere, anywhere, anywhere],
        out_specs=pl.BlockSpec(memory_space=pltpu.VMEM),
        scratch_shapes=[
            pltpu.VMEM((5, SHIFTS * 2, 3 * rows, (ytiles + 2) * SUB, LANES), jnp.float32),
            pltpu.VMEM((count, 3, SUB, LANES), jnp.float32),
            pltpu.VMEM((3, ytiles, 4, rows, SUB, nz), jnp.float32),
            pltpu.VMEM((ytiles, count, rows, SUB, nz), jnp.int32),
            pltpu.VMEM((ytiles, 3, rows, SUB, nz), jnp.float32),
            pltpu.VMEM((ytiles - 1, 3, rows, SUB, nz), jnp.float32),
            pltpu.SemaphoreType.DMA((2,)),
            pltpu.SemaphoreType.DMA((ytiles,)),
            pltpu.SemaphoreType.DMA((40,)),
            pltpu.SemaphoreType.DMA((ytiles, 2)),
            pltpu.SemaphoreType.DMA((ytiles,)),
            pltpu.SemaphoreType.DMA((ytiles, 2)),
            pltpu.SemaphoreType.DMA((ytiles,)),
            pltpu.SemaphoreType.DMA((ytiles,)),
        ],
        compiler_params=pltpu.CompilerParams(
            vmem_limit_bytes=59 << 20, collective_id=0, has_side_effects=True
        ),
        name="bond_step",
    )(offsets.T, displacement, stiffness, intact)
    new_velocity = velocity + change
    new_displacement = displacement + TIME_STEP * new_velocity
    return new_displacement, new_velocity


def solution(mesh):
    return jax.shard_map(
        functools.partial(on_device, mesh.shape["pts"]),
        mesh=mesh,
        in_specs=(
            P(None, "pts", "bond", None),
            P(None, "pts", "bond", None),
            P("pts", "bond", None),
            P("bond", None),
            P("bond", "pts", None, None),
        ),
        out_specs=(P(None, "pts", "bond", None), P(None, "pts", "bond", None)),
        check_vma=False,
    )
```
